256 devices in a mesh: seq: 32 (over y, z), head: 8 (over x, core).
Axes of the slice: x: 4, y: 4, z: 8, core: 2. Of those that a mesh axis runs over, the one named last changes fastest.
Arguments:
- head_inputs: bfloat16 [65536, 5120], P('seq', 'head'), may hold values from -6 to 6
- gate_inputs: bfloat16 [65536, 5120], P('seq', 'head'), may hold values from -6 to 6
- step_raw: bfloat16 [65536, 80], P('seq', 'head'), may hold values from -9 to 2048
- decay_log: float32 [80], replicated, may hold values from -12 to 0
- state_write: bfloat16 [65536, 128], P(('seq', 'head')), may hold values from -6 to 6
- state_read: bfloat16 [65536, 128], P(('seq', 'head')), may hold values from -0.5 to 0.5
- skip_gain: float32 [80], replicated, may hold values from 0.5 to 2
- norm_gain: float32 [5120], replicated, may hold values from 0.1 to 1.9
Outputs:
- scan_output: bfloat16 [65536, 5120], P('seq', 'head')
The draws below stay inside these ranges and needn't reach their ends.
All inputs are finite; a program needn't handle non-finite values.
Results may differ from the reference program's by a relative error of at most 0.005.
Values may be sent and summed in bfloat16 or wider, within the bound.
A program may use at most 128 MiB of HBM per device.

```python
import math
import jax
import jax.numpy as jnp
from jax import lax

HEADS = 80
HEAD_DIM = 64
STATE = 128
SPAN = 256
SEQ = 65536
INNER = 5120


def decay_plan(key):
    base = jax.random.fold_in(key, 4101)
    order = jax.random.permutation(jax.random.fold_in(base, 1), HEADS)
    count = HEADS // 2
    gradual_decay = order < count
    slow_step = jnp.exp(jax.random.uniform(jax.random.fold_in(base, 2), (HEADS,), jnp.float32, jnp.log(0.1 / SEQ), jnp.log(1.0 / SEQ)))
    fast_step = jnp.exp(jax.random.uniform(jax.random.fold_in(base, 3), (HEADS,), jnp.float32, jnp.log(0.02), jnp.log(0.06)))
    per_step = jnp.where(gradual_decay, slow_step, fast_step)
    level = jnp.where(gradual_decay, -5.5, 0.0)
    decay_rate = per_step / jax.nn.softplus(level)
    noise = 0.7 * jax.random.truncated_normal(jax.random.fold_in(base, 4), -3.0, 3.0, (SEQ, HEADS), jnp.float32)
    unscaled_step_sizes = level[None, :] + noise
    chosen_locations = jax.random.randint(jax.random.fold_in(base, 5), (8,), 0, SEQ)
    token_places = jnp.arange(SEQ, dtype=jnp.int32)
    sudden_jump = jnp.any(token_places[:, None] == chosen_locations[None, :], axis=1)
    losses = jax.random.uniform(jax.random.fold_in(base, 6), (SEQ, HEADS), jnp.float32, 0.22, 0.7)
    expected_output = losses / decay_rate[None, :]
    sudden_jump_unscaled = expected_output + jnp.log(-jnp.expm1(-expected_output))
    selected_entries = sudden_jump[:, None] & gradual_decay[None, :]
    unscaled_step_sizes = jnp.where(selected_entries, sudden_jump_unscaled, unscaled_step_sizes)
    scaling = jnp.where(selected_entries, 1.0 / expected_output, 1.0)
    return (unscaled_step_sizes, jnp.log(decay_rate), scaling)


def draw_step_raw(key, part):
    unscaled_step_sizes, decay_logs, scaling = decay_plan(key)
    return unscaled_step_sizes.astype(jnp.bfloat16)


def draw_decay_log(key, part):
    unscaled_step_sizes, decay_logs, scaling = decay_plan(key)
    return decay_logs.astype(jnp.float32)


def draw_head_inputs(key, part):
    unscaled_step_sizes, decay_logs, scaling = decay_plan(key)
    noise = jax.random.truncated_normal(jax.random.fold_in(key, 77), -6.0, 6.0, (SEQ, HEADS, HEAD_DIM), jnp.float32)
    return (noise * scaling[:, :, None]).reshape(SEQ, HEADS * HEAD_DIM).astype(jnp.bfloat16)


def levels(own_key, shape, pieces, low, largest):
    loudness = 1.0
    for axis_at, shards_of in pieces:
        draws = jax.random.uniform(jax.random.fold_in(jax.random.fold_in(own_key, 6), axis_at), (shards_of,), jnp.float32, low / len(pieces), largest / len(pieces))
        loudness = loudness * jnp.repeat(jnp.exp(draws), shape[axis_at] // shards_of).reshape((-1,) + (1,) * (len(shape) - 1 - axis_at))
    return loudness


def centred(rng, extent, scale, most, pieces=(), held_as=jnp.bfloat16):
    drawn = scale * jax.random.normal(rng, extent, jnp.float32)
    if pieces:
        drawn = drawn * levels(rng, extent, pieces, -0.22, 0.18)
    return jnp.clip(drawn, -most, most).astype(held_as)


def setup_inputs(seed: int = 0) -> dict:
    key_list = jax.random.split(jax.random.key(seed), 9)
    return {
        "head_inputs": draw_head_inputs(jax.random.fold_in(key_list[8], 71), 0),
        "gate_inputs": centred(key_list[1], (SEQ, INNER), 1.0, 6.0, ((0, 32), (1, 8))),
        "step_raw": draw_step_raw(jax.random.fold_in(key_list[8], 71), 0),
        "decay_log": draw_decay_log(jax.random.fold_in(key_list[8], 71), 0),
        "state_write": centred(key_list[4], (SEQ, STATE), 1.0, 6.0, ((0, 256),)),
        "state_read": centred(key_list[5], (SEQ, STATE), STATE ** -0.5, 0.5, ((0, 256),)),
        "skip_gain": jnp.clip(jax.random.uniform(key_list[6], (HEADS,), jnp.float32, 0.5, 2.0), 0.5, 2.0),
        "norm_gain": jnp.clip(1.0 + 0.18 * jax.random.normal(key_list[7], (INNER,), jnp.float32), 0.1, 1.9),
    }


def intra_block(values, running, step_size, scores):
    length = running.shape[1]
    row_index = lax.broadcasted_iota(jnp.int32, (length, length), 0)
    col_index = lax.broadcasted_iota(jnp.int32, (length, length), 1)
    lower = col_index <= row_index
    by_head = jnp.moveaxis(running, 2, 1)
    weight_step = jnp.moveaxis(step_size, 2, 1)
    spread = by_head[:, :, :, None] - by_head[:, :, None, :]
    mixing = jnp.where(lower, jnp.exp(jnp.where(lower, spread, 0.0)), 0.0) * scores[:, None] * weight_step[:, :, None, :]
    mixing = lax.optimization_barrier(mixing.astype(jnp.bfloat16)).astype(jnp.float32)
    return jnp.einsum('khtu,kuhp->kthp', mixing, values.astype(jnp.float32))

def block_pieces(values, step_raw, writes, reads, decay_rate, skip_gain):
    tokens = values.shape[0]
    heads = decay_rate.shape[0]
    width = values.shape[1] // heads
    blocks = tokens // SPAN
    group = math.gcd(heads, 4)
    groups = heads // group
    step_size = jax.nn.softplus(step_raw.astype(jnp.float32)).reshape(blocks, SPAN, heads)
    running = jnp.cumsum(-decay_rate * step_size, axis=1)
    shaped = values.reshape(blocks, SPAN, heads, width)
    write_blocks = writes.reshape(blocks, SPAN, -1).astype(jnp.float32)
    read_blocks = reads.reshape(blocks, SPAN, -1).astype(jnp.float32)
    scores = jnp.einsum('ktn,kun->ktu', read_blocks, write_blocks)

    def per_group(item):
        return intra_block(item[0], item[1], item[2], scores)
    split_values = jnp.moveaxis(shaped.reshape(blocks, SPAN, groups, group, width), 2, 0)
    split_running = jnp.moveaxis(running.reshape(blocks, SPAN, groups, group), 2, 0)
    split_step = jnp.moveaxis(step_size.reshape(blocks, SPAN, groups, group), 2, 0)
    mixed_groups = lax.map(per_group, (split_values, split_running, split_step))
    local = jnp.moveaxis(mixed_groups, 0, 2).reshape(blocks, SPAN, heads, width)
    wide_values = shaped.astype(jnp.float32)
    local = local + skip_gain[:, None] * wide_values
    tail = jnp.exp(running[:, -1:, :] - running) * step_size
    weighted = wide_values * tail[..., None]
    weighted = lax.optimization_barrier(weighted.astype(jnp.bfloat16)).astype(jnp.float32)
    states = jnp.einsum('kuhp,kun->khpn', weighted, write_blocks, precision=lax.Precision.HIGHEST)
    return (local, running, states, running[:, -1, :], read_blocks)

def reference(head_inputs, gate_inputs, step_raw, decay_log, state_write, state_read, skip_gain, norm_gain):
    blocks = SEQ // SPAN
    decay_rate = jnp.exp(decay_log)

    def advance(carry, item):
        values, gates, raws, writes, reads = item
        local, running, states, totals, read_blocks = block_pieces(values, raws, writes, reads, decay_rate, skip_gain)
        entering = lax.optimization_barrier(carry.astype(jnp.bfloat16)).astype(jnp.float32)
        inter = jnp.einsum('ktn,hpn->kthp', read_blocks, entering, precision=lax.Precision.HIGHEST)
        ssm = (local + jnp.exp(running)[..., None] * inter).reshape(SPAN, -1)
        gated = ssm * jax.nn.silu(gates.astype(jnp.float32))
        factor = lax.rsqrt(lax.optimization_barrier(jnp.mean(gated * gated, axis=1, keepdims=True)) + 1e-05)
        result = (gated * factor * norm_gain).astype(jnp.bfloat16)
        new_state = jnp.exp(totals[0])[:, None, None] * carry + states[0]
        return (new_state, result)
    items = (head_inputs.reshape(blocks, SPAN, -1), gate_inputs.reshape(blocks, SPAN, -1), step_raw.reshape(blocks, SPAN, -1), state_write.reshape(blocks, SPAN, -1), state_read.reshape(blocks, SPAN, -1))
    start = jnp.zeros((HEADS, HEAD_DIM, STATE), jnp.float32)
    finish, outputs = lax.scan(advance, start, items)
    return outputs.reshape(SEQ, HEADS * HEAD_DIM)
```

```python
import jax
import jax.numpy as jnp
from jax import lax
from jax.experimental import pallas as pl
from jax.experimental.pallas import tpu as pltpu
from jax.sharding import Mesh
from jax.sharding import PartitionSpec as P

HEADS = 80
HEAD_DIM = 64
STATE = 128
INNER = HEADS * HEAD_DIM
EPS = 1e-05

NY, NZ, NX, NC = 4, 8, 4, 2
NH = NX * NC
HL = HEADS // NH
PAIRS = HL // 2
WIDTH = HL * HEAD_DIM
TOKENS = 2048
CH = 128
NCH = TOKENS // CH
BLK = TOKENS // NH
HP = 16
SLICE = STATE // NZ
GROUPS = 2
GCH = NCH // GROUPS

LOG2E = 1.4426950408889634
MESH_ID = pl.DeviceIdType.MESH
F32 = jnp.float32
BF16 = jnp.bfloat16
AXES = ("y", "z", "x", "c")


def mm(a, b, ca=1, cb=0):
    return lax.dot_general(a, b, (((ca,), (cb,)), ((), ())), preferred_element_type=F32)


def split2(v):
    hi = v.astype(BF16)
    return hi, (v - hi.astype(F32)).astype(BF16)


def split3(v):
    hi = v.astype(BF16)
    rest = v - hi.astype(F32)
    mid = rest.astype(BF16)
    return hi, mid, (rest - mid.astype(F32)).astype(BF16)


def kernel(
    x_hbm, z_hbm, raw_hbm, decay_ref, b_hbm, c_hbm, skip_ref, gain_ref, out_ref,
    x_ref, z_ref, raw_ref, b_ref, c_ref, bt_ref, r_ref, q_ref, w_ref, wd_ref,
    tot_ref, off_ref, acc_ref, sb_ref, a_ref, e_ref,
    s_in, p_ref, d_mine, d_all, dl_mine, dl_all, t_mine, t_all, cs_ref, carry_ref, sq_ref,
    load_sem, bs_sem, br_sem, cs_sem, cr_sem, ds_sem, dr_sem, dls_sem, dlr_sem,
    s1_sem, r1_sem, s2_sem, r2_sem, s3_sem, r3_sem, sqs_sem, sqr_sem,
):
    y, z, xx, cc = (lax.axis_index(n) for n in AXES)
    head = xx * NC + cc

    def to(ny=None, nz=None, nx=None, nc=None):
        return (
            y if ny is None else ny,
            z if nz is None else nz,
            xx if nx is None else nx,
            cc if nc is None else nc,
        )

    def remote(src, dst, ssem, rsem, dev):
        return pltpu.make_async_remote_copy(
            src_ref=src, dst_ref=dst, send_sem=ssem, recv_sem=rsem,
            device_id=dev, device_id_type=MESH_ID,
        )

    def rows(slot):
        return pl.ds(pl.multiple_of(slot * BLK, BLK), BLK)

    load_b = pltpu.make_async_copy(b_hbm, b_ref.at[rows(head)], load_sem.at[0])
    load_c = pltpu.make_async_copy(c_hbm, c_ref.at[rows(head)], load_sem.at[1])
    load_raw = pltpu.make_async_copy(raw_hbm, raw_ref, load_sem.at[2])
    load_x = pltpu.make_async_copy(x_hbm, x_ref, load_sem.at[3])
    load_z = pltpu.make_async_copy(z_hbm, z_ref, load_sem.at[4])
    for c in (load_b, load_c, load_raw, load_x, load_z):
        c.start()

    zp = [lax.rem(z + o, NZ) for o in range(1, NZ)]
    zm = [lax.rem(z + NZ - o, NZ) for o in range(1, NZ)]
    yp = [lax.rem(y + o, NY) for o in range(1, NY)]
    ym = [lax.rem(y + NY - o, NY) for o in range(1, NY)]
    hp = [lax.rem(head + o, NH) for o in range(1, NH)]
    hm = [lax.rem(head + NH - o, NH) for o in range(1, NH)]

    barrier = pltpu.get_barrier_semaphore()
    for k in zp:
        pl.semaphore_signal(barrier, inc=1, device_id=to(nz=k), device_id_type=MESH_ID)
    for k in yp:
        pl.semaphore_signal(barrier, inc=1, device_id=to(ny=k), device_id_type=MESH_ID)
    for k in hp:
        pl.semaphore_signal(
            barrier, inc=1, device_id=to(nx=k // NC, nc=lax.rem(k, NC)), device_id_type=MESH_ID
        )
    pl.semaphore_wait(barrier, (NZ - 1) + (NY - 1) + (NH - 1))

    other = 1 - cc
    hops = (1, 3, 2)
    mine = head

    def gather_sends(ref, ssem, rsem):
        out = []
        for i, o in enumerate(hops):
            out.append(remote(
                ref.at[rows(mine)], ref.at[rows(mine)], ssem.at[1 + i], rsem.at[1 + i],
                to(nx=lax.rem(xx + o, NX)),
            ))
        out.append(remote(
            ref.at[rows(mine)], ref.at[rows(mine)], ssem.at[0], rsem.at[0], to(nc=other)
        ))
        return out

    def slot_of(i):
        k = lax.rem(i + 2, 3)
        hop = jnp.where(k == 0, 1, jnp.where(k == 1, 3, 2))
        chip = jnp.where(i == 0, xx, lax.rem(xx + NX - hop, NX))
        core = jnp.where((i >= 1) & (i <= 3), cc, other)
        return chip * NC + core

    def incoming(ref, ssem, rsem, i):
        at = rows(slot_of(i))
        return remote(ref.at[at], ref.at[at], ssem.at[i], rsem.at[i], to(nc=other))

    def forward(ref, ssem, rsem, i):
        at = rows(slot_of(i))
        return remote(ref.at[at], ref.at[at], ssem.at[i + 3], rsem.at[i + 3], to(nc=other))

    load_b.wait()
    b_sends = gather_sends(b_ref, bs_sem, br_sem)
    for c in b_sends:
        c.start()
    load_c.wait()
    c_sends = gather_sends(c_ref, cs_sem, cr_sem)
    for c in c_sends:
        c.start()

    load_raw.wait()
    eye = (
        lax.broadcasted_iota(jnp.int32, (HP, HL), 0) == lax.broadcasted_iota(jnp.int32, (HP, HL), 1)
    ).astype(F32).astype(BF16)
    raw = mm(eye, raw_ref[...], 1, 1)
    step = jnp.maximum(raw, 0.0) + jnp.log1p(jnp.exp(-jnp.abs(raw)))
    sub = lax.broadcasted_iota(jnp.int32, (HP, CH), 0)
    rate = jnp.zeros((HP, CH), F32)
    for h in range(HL):
        rate = jnp.where(sub == h, decay_ref[head * HL + h], rate)
    rate = jnp.where(sub < HL, -LOG2E * jnp.exp(rate), 0.0)
    steps = jnp.concatenate([step[:, k * CH:(k + 1) * CH] for k in range(NCH)], axis=0)
    decays = steps * jnp.concatenate([rate] * NCH, axis=0)
    upper = (
        lax.broadcasted_iota(jnp.int32, (CH, CH), 0) <= lax.broadcasted_iota(jnp.int32, (CH, CH), 1)
    ).astype(F32).astype(BF16)
    hi, mid, lo = split3(decays)
    run = mm(hi, upper) + mm(mid, upper) + mm(lo, upper)
    r_ref[...] = run
    q = run - jnp.log2(steps)
    q_ref[...] = q
    total = jnp.broadcast_to(run[:, CH - 1:CH], (NCH * HP, CH))
    w_ref[...] = jnp.exp2(total - q)
    after = jnp.zeros((HP, CH), F32)
    for k in reversed(range(NCH)):
        at = slice(k * HP, (k + 1) * HP)
        wd_ref[at, :] = jnp.exp2(after + (total[at] - q[at]))
        after = after + total[at]
    left1 = lax.broadcasted_iota(jnp.int32, (1, CH), 1) < HEAD_DIM

    def wide(v):
        return jnp.concatenate(
            [jnp.where(left1, v[2 * p:2 * p + 1], v[2 * p + 1:2 * p + 2]) for p in range(PAIRS)],
            axis=1,
        )

    d_row = wide(after)
    d_mine[...] = d_row
    d_sends = [
        remote(d_mine, d_all.at[z], ds_sem.at[i], dr_sem.at[i], to(nz=k)) for i, k in enumerate(zp)
    ]
    for c in d_sends:
        c.start()
    d_all[z] = d_row
    before = jnp.zeros((HP, CH), F32)
    for k in range(NCH):
        at = slice(k * HP, (k + 1) * HP)
        tot_ref[k] = jnp.exp2(wide(total[at]))
        off_ref[k] = jnp.exp2(wide(before))
        before = before + total[at]

    acc_ref[...] = jnp.zeros_like(acc_ref)
    left = lax.broadcasted_iota(jnp.int32, (CH, CH), 1) < HEAD_DIM
    load_x.wait()

    def add_block(slot):
        at = rows(slot)
        bt0 = b_ref[pl.ds(pl.multiple_of(slot * BLK, BLK), CH), :].astype(F32).T
        bt1 = b_ref[pl.ds(pl.multiple_of(slot * BLK + CH, CH), CH), :].astype(F32).T
        bt_ref[2 * slot] = bt0
        bt_ref[2 * slot + 1] = bt1
        base = pl.multiple_of(slot * 2 * HP, 2 * HP)
        w0 = wd_ref[pl.ds(base, HP), :]
        w1 = wd_ref[pl.ds(base + HP, HP), :]
        for p in range(PAIRS):
            cols = slice(p * CH, (p + 1) * CH)
            lhs = jnp.concatenate(
                [
                    jnp.concatenate(
                        [
                            (bt0 * w0[h:h + 1]).astype(BF16),
                            (bt1 * w1[h:h + 1]).astype(BF16),
                        ],
                        axis=1,
                    )
                    for h in (2 * p, 2 * p + 1)
                ],
                axis=0,
            )
            o = mm(lhs, x_ref[at, cols])
            acc_ref[:, cols] += jnp.where(left, o[:CH], o[CH:])

    add_block(mine)

    def gathered(i, _):
        incoming(b_ref, bs_sem, br_sem, i).wait_recv()

        @pl.when((i >= 1) & (i <= 3))
        def _():
            forward(b_ref, bs_sem, br_sem, i).start()

        add_block(slot_of(i))
        return 0

    lax.fori_loop(0, NH - 1, gathered, 0)

    def slc(k):
        return pl.ds(pl.multiple_of(k * SLICE, SLICE), SLICE)

    sb_ref[...] = acc_ref[...].astype(BF16)
    s_sends = [
        remote(sb_ref.at[slc(k)], s_in.at[z], s1_sem.at[i], r1_sem.at[i], to(nz=k))
        for i, k in enumerate(zp)
    ]
    for c in s_sends:
        c.start()
    s_in[z] = sb_ref[slc(z), :]

    for i, k in enumerate(zm):
        remote(d_mine, d_all.at[k], ds_sem.at[i], dr_sem.at[i], to(nz=k)).wait_recv()
    line = d_all[0]
    for k in range(1, NZ):
        line = line + d_all[k]
    dl_mine[...] = line
    dl_sends = [
        remote(dl_mine, dl_all.at[y], dls_sem.at[i], dlr_sem.at[i], to(ny=k))
        for i, k in enumerate(yp)
    ]
    for c in dl_sends:
        c.start()
    dl_all[y] = line

    for i in range(1, 4):
        incoming(c_ref, cs_sem, cr_sem, i).wait_recv()
        forward(c_ref, cs_sem, cr_sem, i).start()
    load_z.wait()
    for i in (0, 4, 5, 6):
        incoming(c_ref, cs_sem, cr_sem, i).wait_recv()

    acc_ref[...] = jnp.zeros_like(acc_ref)
    cap = jnp.where(
        lax.broadcasted_iota(jnp.int32, (CH, CH), 0) >= lax.broadcasted_iota(jnp.int32, (CH, CH), 1),
        1e3, -1e30,
    )

    def chunk(k, _):
        at = pl.ds(pl.multiple_of(k * CH, CH), CH)
        hat = pl.ds(pl.multiple_of(k * HP, HP), HP)
        bk, ck = b_ref[at, :], c_ref[at, :]
        scores = mm(ck, bk, 1, 1)
        bt = bt_ref[k]
        rc = r_ref[hat, :].T
        qk, wk = q_ref[hat, :], w_ref[hat, :]
        tot, off = tot_ref[k], off_ref[k]
        for p in range(PAIRS):
            cols = slice(p * CH, (p + 1) * CH)
            mix, ws, rb = [], [], []
            for h in (2 * p, 2 * p + 1):
                r = jnp.broadcast_to(rc[:, h:h + 1], (CH, CH))
                rb.append(r)
                m = jnp.exp2(jnp.minimum(r - qk[h:h + 1], cap)) * scores
                mix.append(m.astype(BF16))
                ws.append((bt * wk[h:h + 1]).astype(BF16))
            lhs = jnp.concatenate(
                [jnp.concatenate(mix, axis=1), jnp.concatenate(ws, axis=1)], axis=0
            )
            xp = x_ref[at, cols]
            zero = jnp.zeros_like(xp)
            rhs = jnp.concatenate([jnp.where(left, xp, zero), jnp.where(left, zero, xp)], axis=0)
            o = mm(lhs, rhs)
            state = acc_ref[:, cols]
            inter = mm(ck, state.astype(BF16))
            er = jnp.exp2(jnp.where(left, rb[0], rb[1]))
            first = head * HL + 2 * p
            skip = jnp.where(left1, skip_ref[first], skip_ref[first + 1])
            zv = z_ref[at, cols].astype(F32)
            gate = zv * (0.5 + 0.5 * jnp.tanh(0.5 * zv))
            a_ref[at, cols] = (o[:CH] + er * inter + skip * xp.astype(F32)) * gate
            e_ref[at, cols] = er * gate * off[:, cols]
            acc_ref[:, cols] = state * tot[:, cols] + o[CH:]
        return 0

    lax.fori_loop(0, 6, chunk, 0)

    for i, k in enumerate(zm):
        remote(sb_ref.at[slc(k)], s_in.at[k], s1_sem.at[i], r1_sem.at[i], to(nz=k)).wait_recv()
    pre = jnp.zeros((SLICE, WIDTH), F32)
    for k in range(NZ):
        p_ref[k] = pre
        pre = pre * jnp.exp2(d_all[k]) + s_in[k].astype(F32)
    t_mine[...] = pre.astype(BF16)
    t_sends = [
        remote(t_mine, t_all.at[y], s2_sem.at[i], r2_sem.at[i], to(ny=k)) for i, k in enumerate(yp)
    ]
    for c in t_sends:
        c.start()
    t_all[y] = pre.astype(BF16)

    lax.fori_loop(6, 10, chunk, 0)

    for i, k in enumerate(ym):
        remote(dl_mine, dl_all.at[k], dls_sem.at[i], dlr_sem.at[i], to(ny=k)).wait_recv()
        remote(t_mine, t_all.at[k], s2_sem.at[i], r2_sem.at[i], to(ny=k)).wait_recv()
    into = jnp.zeros((SLICE, WIDTH), F32)
    for k in range(NY - 1):
        into = jnp.where(k < y, into * jnp.exp2(dl_all[k]) + t_all[k].astype(F32), into)
    upto = jnp.zeros((1, WIDTH), F32)
    for k in range(NZ):
        cs_ref[k] = (p_ref[k] + jnp.exp2(upto) * into).astype(BF16)
        upto = upto + d_all[k]
    k_sends = [
        remote(cs_ref.at[k], carry_ref.at[slc(z)], s3_sem.at[i], r3_sem.at[i], to(nz=k))
        for i, k in enumerate(zp)
    ]
    for c in k_sends:
        c.start()
    carry_ref[slc(z), :] = cs_ref[z]

    lax.fori_loop(10, NCH, chunk, 0)

    for i, k in enumerate(zm):
        remote(cs_ref.at[k], carry_ref.at[slc(k)], s3_sem.at[i], r3_sem.at[i], to(nz=k)).wait_recv()

    ones8 = jnp.ones((8, 2 * CH), F32).astype(BF16)

    def finish(k, _):
        at = pl.ds(pl.multiple_of(k * CH, CH), CH)
        ck = c_ref[at, :]
        part = jnp.zeros((CH, CH), F32)
        for p in range(PAIRS):
            cols = slice(p * CH, (p + 1) * CH)
            g = a_ref[at, cols] + e_ref[at, cols] * mm(ck, carry_ref[:, cols])
            a_ref[at, cols] = g
            part = part + g * g
        s = mm(ones8, jnp.concatenate(split2(part), axis=1), 1, 1)
        sq_ref[k, head] = s[0:1]
        return 0

    def group(g):
        return pl.ds(g * GCH, GCH)

    q_sends = []
    for g in range(GROUPS):
        lax.fori_loop(g * GCH, (g + 1) * GCH, finish, 0)
        for i, k in enumerate(hp):
            c = remote(
                sq_ref.at[group(g), head], sq_ref.at[group(g), head], sqs_sem.at[g, i], sqr_sem.at[g, i],
                to(nx=k // NC, nc=lax.rem(k, NC)),
            )
            c.start()
            q_sends.append(c)

    ones16 = jnp.ones((2 * NH, CH), F32).astype(BF16)
    gains = [gain_ref[pl.ds(head * PAIRS + p, 1), :] for p in range(PAIRS)]

    def scale(k, _):
        at = pl.ds(pl.multiple_of(k * CH, CH), CH)
        hi, lo = split2(sq_ref[k].reshape(NH, CH))
        both = jnp.concatenate([hi.astype(F32), lo.astype(F32)], axis=0).astype(BF16)
        s = mm(both, ones16, 0, 0)
        f = lax.rsqrt(s * (1.0 / INNER) + EPS)
        for p in range(PAIRS):
            cols = slice(p * CH, (p + 1) * CH)
            out_ref[at, cols] = (a_ref[at, cols] * f * gains[p]).astype(BF16)
        return 0

    for g in range(GROUPS):
        for i, k in enumerate(hm):
            remote(
                sq_ref.at[group(g), k], sq_ref.at[group(g), k], sqs_sem.at[g, i], sqr_sem.at[g, i],
                to(nx=k // NC, nc=lax.rem(k, NC)),
            ).wait_recv()
        lax.fori_loop(g * GCH, (g + 1) * GCH, scale, 0)

    for c in b_sends + c_sends + d_sends + s_sends + dl_sends + t_sends + k_sends + q_sends:
        c.wait_send()
    for i in range(1, 4):
        forward(b_ref, bs_sem, br_sem, i).wait_send()
        forward(c_ref, cs_sem, cr_sem, i).wait_send()


def on_device(x, zg, raw, decay, b, c, skip, gain):
    any_ = pl.BlockSpec(memory_space=pl.ANY)
    smem = pl.BlockSpec(memory_space=pltpu.SMEM)
    vmem = pl.BlockSpec(memory_space=pltpu.VMEM)
    dma = pltpu.SemaphoreType.DMA
    v = pltpu.VMEM
    return pl.pallas_call(
        kernel,
        out_shape=jax.ShapeDtypeStruct((TOKENS, WIDTH), BF16),
        in_specs=[any_, any_, any_, smem, any_, any_, smem, vmem],
        out_specs=vmem,
        scratch_shapes=[
            v((TOKENS, WIDTH), BF16),
            v((TOKENS, WIDTH), BF16),
            v((TOKENS, HL), BF16),
            v((TOKENS, STATE), BF16),
            v((TOKENS, STATE), BF16),
            v((NCH, STATE, CH), F32),
            v((NCH * HP, CH), F32),
            v((NCH * HP, CH), F32),
            v((NCH * HP, CH), F32),
            v((NCH * HP, CH), F32),
            v((NCH, 1, WIDTH), F32),
            v((NCH, 1, WIDTH), F32),
            v((STATE, WIDTH), F32),
            v((STATE, WIDTH), BF16),
            v((TOKENS, WIDTH), F32),
            v((TOKENS, WIDTH), F32),
            v((NZ, SLICE, WIDTH), BF16),
            v((NZ, SLICE, WIDTH), F32),
            v((1, WIDTH), F32),
            v((NZ, 1, WIDTH), F32),
            v((1, WIDTH), F32),
            v((NY, 1, WIDTH), F32),
            v((SLICE, WIDTH), BF16),
            v((NY, SLICE, WIDTH), BF16),
            v((NZ, SLICE, WIDTH), BF16),
            v((STATE, WIDTH), BF16),
            v((NCH, NH, 1, CH), F32),
            dma((5,)),
            dma((NH - 1,)), dma((NH - 1,)),
            dma((NH - 1,)), dma((NH - 1,)),
            dma((NZ - 1,)), dma((NZ - 1,)),
            dma((NY - 1,)), dma((NY - 1,)),
            dma((NZ - 1,)), dma((NZ - 1,)),
            dma((NY - 1,)), dma((NY - 1,)),
            dma((NZ - 1,)), dma((NZ - 1,)),
            dma((GROUPS, NH - 1)), dma((GROUPS, NH - 1)),
        ],
        compiler_params=pltpu.CompilerParams(
            collective_id=0, has_side_effects=True, vmem_limit_bytes=48 * 1024 * 1024
        ),
        name="ssd",
    )(x, zg, raw, decay, b, c, skip, gain.reshape(INNER // CH, CH))


def solution(mesh):
    finer = Mesh(mesh.devices.reshape(NY, NZ, NX, NC), AXES)
    seq, head = ("y", "z"), ("x", "c")
    placed = (
        P(seq, head), P(seq, head), P(seq, head), P(),
        P(seq + head, None), P(seq + head, None), P(), P(),
    )
    return jax.shard_map(
        on_device, mesh=finer, in_specs=placed, out_specs=P(seq, head), check_vma=False
    )
```
